32 devices in a mesh: rad: 4 (over z), ma: 8 (over y, x, core).
Axes of the slice: x: 2, y: 2, z: 4, core: 2. Of those that a mesh axis runs over, the one named last changes fastest.
Arguments:
- spectra: bfloat16 [32, 3, 2, 1024, 1024], P(('rad', 'ma')), may hold values from -0.19921875 to 0.19921875
- legendre: bfloat16 [1024, 1024, 512], P('ma', 'rad'), may hold values from -0.1875 to 0.1875
- selected: int32 [16], replicated, may hold values from 0 to 31, as said below
- m_order: int32 [1024], replicated, may hold values from 0 to 1023, each once
Outputs:
- shell_grid: float32 [16, 3, 2, 512, 3072], P(None, None, None, ('rad', 'ma'))
The draws below stay inside these ranges and needn't reach their ends.
Inputs may be any that keep to these rules, and one draw needn't show every extreme that they name: `selected`: 16 distinct radii, in no particular order. `m_order`: every wavenumber 0 to 1023 stands in exactly one slot.
All inputs are finite; a program needn't handle non-finite values.
Results may differ from the reference program's by a relative error of at most 0.012.
Values may be sent and summed in bfloat16 or wider, within the bound.
No kernel may reach another device: no remote copies, remote signals or barrier semaphores. Data moves between devices by JAX's collectives and lax.ppermute only.
A program may use at most 192 MiB of HBM per device.

```python
import jax
import jax.numpy as jnp
from jax import lax

L = 1024
M = 1024
NPHI = 3072
FIELDS = 3
SEL = 16
R = 32
NTHH = 512
N_RAD = 4


def draw_selected(key, part):
    return jax.random.permutation(key, R)[:SEL].astype(jnp.int32)


def level_of(stream_key, extent, split, least, high):
    factor_of = 1.0
    for position, parts in split:
        draws = jax.random.uniform(jax.random.fold_in(jax.random.fold_in(stream_key, 6), position), (parts,), jnp.float32, least / len(split), high / len(split))
        factor_of = factor_of * jnp.repeat(jnp.exp(draws), extent[position] // parts).reshape((-1,) + (1,) * (len(extent) - 1 - position))
    return factor_of


def centred(rng, dims, deviation, reach, pieces=(), kind=jnp.bfloat16):
    factor_of = level_of(rng, dims, pieces, -0.22, 0.18) if pieces else 1.0
    drawn = jax.random.normal(rng, dims, jnp.float32) * deviation * factor_of
    return jnp.minimum(jnp.maximum(drawn, -reach), reach).astype(kind)


def setup_inputs(seed: int = 0) -> dict:
    keys = jax.random.split(jax.random.key(seed), 5)
    return {
        "spectra": centred(keys[0], (R, FIELDS, 2, M, L), 0.03, 0.19921875, ((0, 32),)),
        "legendre": centred(keys[1], (M, L, NTHH), L ** -0.5, 0.1875, ((0, 8), (1, 4))),
        "selected": draw_selected(jax.random.fold_in(keys[4], 71), 0),
        "m_order": jax.random.permutation(keys[3], M).astype(jnp.int32),
    }


def reference(spectra, legendre, selected, m_order):
    picked = spectra[selected]
    picked = picked[:, :, :, m_order, :]
    degree = jnp.arange(L, dtype=jnp.int32)
    tri_mask = degree[None, :] >= m_order[:, None]
    picked = jnp.where(tri_mask[None, None, None], picked, jnp.zeros((), jnp.bfloat16))
    width = SEL * FIELDS * 2
    coeffs = picked.reshape(width, M, L).transpose(1, 0, 2)
    m_sign = (1 - 2 * (m_order % 2)).astype(jnp.float32)
    part_len = L // N_RAD
    total = jnp.zeros((2, M, width, NTHH), jnp.float32)
    for part_index in range(N_RAD):
        first = part_index * part_len
        block = coeffs[:, :, first:first + part_len].astype(jnp.float32)
        ptab = legendre[:, first:first + part_len, :].astype(jnp.float32)
        even_sum = jnp.einsum('sil,slt->sit', block[:, :, 0::2], ptab[:, 0::2, :])
        odd_sum = jnp.einsum('sil,slt->sit', block[:, :, 1::2], ptab[:, 1::2, :])
        north_sum = (even_sum + odd_sum).astype(jnp.bfloat16)
        south_sum = (m_sign[:, None, None] * (even_sum - odd_sum)).astype(jnp.bfloat16)
        north_sum, south_sum = lax.optimization_barrier((north_sum, south_sum))
        total = total + jnp.stack([north_sum.astype(jnp.float32), south_sum.astype(jnp.float32)])
    latitude_sum = total.astype(jnp.bfloat16)
    arranged = latitude_sum.reshape(2, M, SEL, FIELDS, 2, NTHH).transpose(2, 3, 0, 5, 4, 1)
    arranged = arranged.reshape(SEL * FIELDS * 2 * NTHH, 2 * M)
    phase = (m_order[:, None] * jnp.arange(NPHI, dtype=jnp.int32)[None, :]) % NPHI
    angle = phase.astype(jnp.float32) * (2.0 * jnp.pi / NPHI)
    weight = jnp.where(m_order == 0, 1.0, 2.0).astype(jnp.float32)
    dft_table = jnp.concatenate([weight[:, None] * jnp.cos(angle), -weight[:, None] * jnp.sin(angle)], axis=0).astype(jnp.bfloat16)
    grid = jnp.dot(arranged.astype(jnp.float32), dft_table.astype(jnp.float32), preferred_element_type=jnp.float32)
    return grid.reshape(SEL, FIELDS, 2, NTHH, NPHI)
```

```python
import jax
import jax.numpy as jnp
from jax import lax
from jax.sharding import PartitionSpec as P

CHUNKS = 4


def local(spectra, legendre, selected, m_order):
    rad_count = lax.axis_size("rad")
    ma_count = lax.axis_size("ma")
    rad_index = lax.axis_index("rad")
    ma_index = lax.axis_index("ma")
    slot_count, part_len, rows = legendre.shape
    band_rows = rows // rad_count
    row_block = band_rows // ma_count
    owned, fields, parts, m_total, l_total = spectra.shape
    nphi = 3 * m_total
    channels = fields * parts
    sel = selected.shape[0]
    width = sel * channels
    plane = ma_count * owned
    piece = slot_count // CHUNKS

    radii = jnp.arange(rad_count * plane, dtype=jnp.int32)
    wanted = (selected[:, None] == radii[None, :]).any(axis=0).reshape(rad_count, plane)
    counts = wanted.sum(axis=1).astype(jnp.int32)
    order = jnp.argsort(jnp.where(wanted, 0, 1), axis=1, stable=True).astype(jnp.int32)
    rank = (jnp.cumsum(wanted.astype(jnp.int32), axis=1) - 1).reshape(-1)[selected]
    sel_plane = selected // plane
    mine = lax.dynamic_index_in_dim(order, rad_index, 0, keepdims=False)

    slot_m = lax.dynamic_slice_in_dim(m_order, ma_index * slot_count, slot_count)
    degree = rad_index * part_len + jnp.arange(part_len, dtype=jnp.int32)
    mask = (degree[None, :] >= slot_m[:, None]).astype(jnp.bfloat16)
    m_sign = (1 - 2 * (slot_m % 2)).astype(jnp.bfloat16)
    parity = m_sign[:, None] * (1 - 2 * (degree % 2)).astype(jnp.bfloat16)[None, :]

    flat = spectra.reshape(owned * channels * m_total, l_total)
    lead = jnp.arange(owned * channels, dtype=jnp.int32) * m_total
    slots = m_order.reshape(ma_count, CHUNKS, piece)

    def synth(blocks, table, first):
        lhs = jnp.concatenate(blocks, axis=3)
        count = lhs.shape[3]
        lhs = lhs.reshape(ma_count, row_block, 2, count, sel, fields, 2)
        lhs = lhs.transpose(4, 5, 2, 1, 6, 0, 3).reshape(-1, 2 * ma_count * count)
        lo = first * piece
        rhs = table.reshape(2, ma_count, slot_count, nphi)[:, :, lo : lo + count]
        rhs = rhs.reshape(2 * ma_count * count, nphi)
        return jnp.dot(lhs, rhs, preferred_element_type=jnp.float32)

    def run(cap):
        def body(flat, legendre, m_order):
            phase = m_order[:, None] * jnp.arange(nphi, dtype=jnp.int32)[None, :] % nphi
            angle = phase.astype(jnp.float32) * (2.0 * jnp.pi / nphi)
            weight = jnp.where(m_order == 0, 1.0, 2.0).astype(jnp.float32)
            table = jnp.concatenate(
                [weight[:, None] * jnp.cos(angle), -weight[:, None] * jnp.sin(angle)], axis=0
            ).astype(jnp.bfloat16)
            landed = []
            tie = None
            for k in range(CHUNKS):
                rows_k = lead[None, :, None] + slots[:, k][:, None, :]
                out = jnp.take(flat, rows_k.reshape(-1), axis=0, mode="clip")
                out = out.reshape(ma_count, owned * channels, piece, l_total)
                if tie is not None:
                    out, tie = lax.optimization_barrier((out, tie))
                near = lax.all_to_all(out, "ma", split_axis=0, concat_axis=0, tiled=True)
                near = near.reshape(plane, channels, piece, l_total)
                send = jnp.take(near, mine[:cap], axis=0, mode="clip")
                send = send.reshape(cap, channels, piece, rad_count, part_len)
                send = send.transpose(3, 0, 1, 2, 4)
                got = lax.all_to_all(send, "rad", split_axis=0, concat_axis=0, tiled=True)
                tie = got
                got = got.reshape(rad_count * cap, channels, piece, part_len)
                coeffs = jnp.take(got, sel_plane * cap + rank, axis=0, mode="clip")
                coeffs = coeffs.reshape(width, piece, part_len).transpose(1, 0, 2)
                lo = k * piece
                inside = mask[lo : lo + piece, None, :] != 0
                coeffs = jnp.where(inside, coeffs, jnp.zeros((), jnp.bfloat16))
                flipped = coeffs * parity[lo : lo + piece, None, :]
                leg = legendre[lo : lo + piece]
                north = jnp.einsum("slt,sil->tsi", leg, coeffs, preferred_element_type=jnp.float32)
                south = jnp.einsum("slt,sil->tsi", leg, flipped, preferred_element_type=jnp.float32)
                both = jnp.stack([north.astype(jnp.bfloat16), south.astype(jnp.bfloat16)], axis=1)
                both = both.reshape(rows, 2 * piece * width)
                if k == CHUNKS - 1:
                    both, table = lax.optimization_barrier((both, table))
                band = lax.psum_scatter(
                    both, "rad", scatter_dimension=0, tiled=True
                )
                if k == CHUNKS - 1:
                    grid = synth(landed, table, 0)
                    band, grid = lax.optimization_barrier((band, grid))
                pieces = lax.all_to_all(
                    band.reshape(ma_count, row_block, 2 * piece * width),
                    "ma", split_axis=0, concat_axis=0, tiled=True,
                )
                landed.append(pieces.reshape(ma_count, row_block, 2, piece, width))
            grid = grid + synth(landed[-1:], table, CHUNKS - 1)
            return grid.reshape(sel, fields, 2, row_block, nphi)

        return body

    most = min(sel, plane)
    fair = -(-sel // rad_count)
    caps = sorted({min(most, fair + 2), most})
    level = jnp.int32(0)
    for cap in caps[:-1]:
        level = level + (counts.max() > cap).astype(jnp.int32)
    return lax.switch(level, [run(cap) for cap in caps], flat, legendre, m_order)


def solution(mesh):
    return jax.shard_map(
        local,
        mesh=mesh,
        in_specs=(P(("rad", "ma"), None, None, None, None), P("ma", "rad", None), P(), P()),
        out_specs=P(None, None, None, ("rad", "ma"), None),
        check_vma=False,
    )
```
